32 devices in a mesh: ka: 16 (over z, x, core), sp: 2 (over y).
Axes of the slice: x: 2, y: 2, z: 4, core: 2. Of those that a mesh axis runs over, the one named last changes fastest.
Arguments:
- bloch_index: int32 [16, 2], P('ka'), may hold values from 0 to 63
- material: int32 [32, 64, 128], P('sp'), may hold values from 0 to 2
- permittivity: float32 [3], replicated, may hold values from 1 to 12
- absorption_peak: float32 [1], replicated, may hold values from 0.25 to 2
- source_sheet: float32 [16, 2, 32, 64], P('ka', None, 'sp'), may hold values from -6 to 6
- waveform: float32 [10], replicated, may hold values from -6 to 6
- electric_in: bfloat16 [16, 6, 32, 64, 128], P('ka', None, 'sp'), may hold values from -12 to 12
- magnetic_in: bfloat16 [16, 6, 32, 64, 128], P('ka', None, 'sp'), may hold values from -12 to 12
Outputs:
- electric_out: float32 [16, 6, 32, 64, 128], P('ka', None, 'sp')
- magnetic_out: float32 [16, 6, 32, 64, 128], P('ka', None, 'sp')
- reflected: float32 [16, 2], P('ka')
- reflected_mean: float32 [2], replicated
The draws below stay inside these ranges and needn't reach their ends.
All inputs are finite; a program needn't handle non-finite values.
Results may differ from the reference program's by a relative error of at most 0.0003.
Values sent between devices are 32-bit elements; how exact they have to be, the bound alone decides.
A program may use at most 64 MiB of HBM per device.

```python
import math
import jax
import jax.numpy as jnp
from jax import lax

NY = 64
NZ = 128
PML = 16
STEPS = 10
INTERVAL = 5
NSNAP = 2
MPHASE = 64
NMAT = 3
K = 16
NX = 32


def start_field(key, salt):
    key = jax.random.fold_in(key, salt)
    level_key, phase_key, noise_key, common_key = jax.random.split(key, 4)
    level = jax.random.uniform(level_key, (K, 1, 1, 1, 1), jnp.float32, -1.0, 1.0)
    amplitude = jnp.exp(0.6931472 * level)
    phase = jax.random.uniform(phase_key, (K, 1, 1, 1, 1), jnp.float32, 0.0, 6.2831853)
    across = jnp.arange(NX, dtype=jnp.float32).reshape(1, 1, NX, 1, 1)
    profile = 1.0 + 0.6 * jnp.sin(6.2831853 * across / NX + phase)
    full_shape = (K, 6, NX, NY, NZ)
    rough = jnp.clip(jax.random.normal(noise_key, full_shape, jnp.float32), -3.5, 3.5)
    return (amplitude * profile * rough).astype(jnp.bfloat16)


def draw_electric_in(key, part):
    return start_field(key, 11)


def draw_magnetic_in(key, part):
    return start_field(key, 23)


def set_ends(values, rng, low, top_value):
    longest = values.shape.index(max(values.shape))
    spots = []
    for shift in (0, 1):
        where = [jax.random.randint(jax.random.fold_in(rng, axis), (), 0, length) for axis, length in enumerate(values.shape)]
        where[longest] = (where[longest] + shift) % values.shape[longest]
        spots.append(tuple(where))
    return values.at[spots[0]].set(low).at[spots[1]].set(top_value)


def block_scale(rng, dims, cuts, low, largest):
    gain = 1.0
    for position, blocks in cuts:
        heights = jax.random.uniform(jax.random.fold_in(jax.random.fold_in(rng, 6), position), (blocks,), jnp.float32, low / len(cuts), largest / len(cuts))
        gain = gain * jnp.repeat(jnp.exp(heights), dims[position] // blocks).reshape((-1,) + (1,) * (len(dims) - 1 - position))
    return gain


def normal_values(stream_key, extent, deviation, reach, shards=(), kind=jnp.bfloat16):
    values = deviation * jax.random.normal(stream_key, extent, jnp.float32)
    if shards:
        values = values * block_scale(stream_key, extent, shards, -0.22, 0.18)
    return jnp.clip(values, -reach, reach).astype(kind)


def setup_inputs(seed: int = 0) -> dict:
    keys = jax.random.split(jax.random.key(seed), 9)
    bloch_index = set_ends(jax.random.randint(keys[0], (K, 2), 0, MPHASE), jax.random.fold_in(keys[0], 1), 0, MPHASE - 1).astype(jnp.int32)
    material = set_ends(jax.random.randint(keys[1], (NX, NY, NZ), 0, NMAT), jax.random.fold_in(keys[1], 1), 0, NMAT - 1).astype(jnp.int32)
    permittivity = jnp.clip(jnp.exp(jax.random.uniform(keys[2], (NMAT,), jnp.float32, math.log(1.0), math.log(12.0))), 1.0, 12.0)
    absorption_peak = jnp.clip(jnp.exp(jax.random.uniform(keys[3], (1,), jnp.float32, math.log(0.25), math.log(2.0))), 0.25, 2.0)
    source_sheet = normal_values(keys[4], (K, 2, NX, NY), 1.0, 6.0, ((0, 16), (2, 2)), jnp.float32)
    waveform = normal_values(keys[5], (STEPS,), 1.0, 6.0, (), jnp.float32)
    electric_in = draw_electric_in(jax.random.fold_in(keys[8], 71), 0)
    magnetic_in = draw_magnetic_in(jax.random.fold_in(keys[8], 71), 0)
    return dict(bloch_index=bloch_index, material=material, permittivity=permittivity, absorption_peak=absorption_peak, source_sheet=source_sheet, waveform=waveform, electric_in=electric_in, magnetic_in=magnetic_in)


TIME_STEP = 0.5


def rotate(couple, cosine, sine):
    return (couple[0] * cosine - couple[1] * sine, couple[0] * sine + couple[1] * cosine)


def subtract(left, right):
    return (left[0] - right[0], left[1] - right[1])


def slice_along(couple, begin_at, end_at, along):
    return tuple(lax.slice_in_dim(values, begin_at, end_at, axis=along) for values in couple)


def attach(front, back, along):
    return tuple(jnp.concatenate([first_part, second_part], axis=along) for first_part, second_part in zip(front, back))


def above_cell(couple, beyond, along):
    length = couple[0].shape[along]
    return attach(slice_along(couple, 1, length, along), beyond, along)


def below_cell(couple, beyond, along):
    length = couple[0].shape[along]
    return attach(beyond, slice_along(couple, 0, length - 1, along), along)


def forward_wrap(couple, along, cosine, sine):
    beyond = rotate(slice_along(couple, 0, 1, along), cosine, sine)
    return subtract(above_cell(couple, beyond, along), couple)


def backward_wrap(couple, along, cosine, sine):
    length = couple[0].shape[along]
    beyond = rotate(slice_along(couple, length - 1, length, along), cosine, -sine)
    return subtract(couple, below_cell(couple, beyond, along))


def forward_open(couple):
    along = couple[0].ndim - 1
    beyond = tuple(jnp.zeros_like(values) for values in slice_along(couple, 0, 1, along))
    return subtract(above_cell(couple, beyond, along), couple)


def backward_open(couple):
    along = couple[0].ndim - 1
    beyond = tuple(jnp.zeros_like(values) for values in slice_along(couple, 0, 1, along))
    return subtract(couple, below_cell(couple, beyond, along))


def electric_curl(electric, beyond_y, beyond_z, cosine, sine):
    ex_part, ey_part, ez_part = electric
    across = ex_part[0].ndim - 3
    sideways = across + 1
    dx_ey = subtract(above_cell(ey_part, beyond_y, across), ey_part)
    dx_ez = subtract(above_cell(ez_part, beyond_z, across), ez_part)
    return (subtract(forward_wrap(ez_part, sideways, cosine, sine), forward_open(ey_part)),
            subtract(forward_open(ex_part), dx_ez),
            subtract(dx_ey, forward_wrap(ex_part, sideways, cosine, sine)))


def magnetic_curl(magnetic, behind_y, behind_z, cosine, sine):
    hx_part, hy_part, hz_part = magnetic
    across = hx_part[0].ndim - 3
    sideways = across + 1
    bx_hy = subtract(hy_part, below_cell(hy_part, behind_y, across))
    bx_hz = subtract(hz_part, below_cell(hz_part, behind_z, across))
    return (subtract(backward_wrap(hz_part, sideways, cosine, sine), backward_open(hy_part)),
            subtract(backward_open(hx_part), bx_hz),
            subtract(bx_hy, backward_wrap(hx_part, sideways, cosine, sine)))


def relax(couple, change, retain, factor):
    return (retain * couple[0] + factor * change[0], retain * couple[1] + factor * change[1])


def coefficients(material, permittivity, absorption_peak, depth):
    height = jnp.arange(depth, dtype=jnp.float32)
    low_depth = jnp.maximum(PML - height, 0.0) / PML
    high_depth = jnp.maximum(height - (depth - 1 - PML), 0.0) / PML
    conduct = absorption_peak[0] * (low_depth ** 3 + high_depth ** 3)
    half_mag = conduct * (0.5 * TIME_STEP)
    h_retain = (1.0 - half_mag) / (1.0 + half_mag)
    h_factor = -TIME_STEP / (1.0 + half_mag)
    relative = jnp.zeros(material.shape, jnp.float32)
    for level in range(NMAT):
        relative = relative + jnp.where(material == level, permittivity[level], 0.0)
    half_ele = conduct * (0.5 * TIME_STEP) / relative
    e_retain = (1.0 - half_ele) / (1.0 + half_ele)
    e_factor = TIME_STEP / relative / (1.0 + half_ele)
    return e_retain, e_factor, h_retain, h_factor


def reference(bloch_index, material, permittivity, absorption_peak, source_sheet, waveform, electric_in, magnetic_in):
    depth = material.shape[2]
    rows = material.shape[0]
    e_retain, e_factor, h_retain, h_factor = coefficients(material, permittivity, absorption_peak, depth)
    plane = (jnp.arange(depth) == PML + 2).astype(jnp.float32)
    monitor = PML + 6
    angles = 2.0 * jnp.pi * bloch_index.astype(jnp.float32) / MPHASE

    def one_point(inputs):
        angle_pair, sheet_pair, electric_begin, magnetic_begin = inputs
        cos_x = jnp.cos(angle_pair[0])
        sin_x = jnp.sin(angle_pair[0])
        cos_y = jnp.cos(angle_pair[1])
        sin_y = jnp.sin(angle_pair[1])
        sheet = (sheet_pair[0][:, :, None] * plane, sheet_pair[1][:, :, None] * plane)

        def advance(fields, drive):
            electric, magnetic = fields
            beyond_y = rotate(slice_along(electric[1], 0, 1, 0), cos_x, sin_x)
            beyond_z = rotate(slice_along(electric[2], 0, 1, 0), cos_x, sin_x)
            change = electric_curl(electric, beyond_y, beyond_z, cos_y, sin_y)
            magnetic = tuple(relax(couple, change_part, h_retain, h_factor) for couple, change_part in zip(magnetic, change))
            behind_y = rotate(slice_along(magnetic[1], rows - 1, rows, 0), cos_x, -sin_x)
            behind_z = rotate(slice_along(magnetic[2], rows - 1, rows, 0), cos_x, -sin_x)
            change = magnetic_curl(magnetic, behind_y, behind_z, cos_y, sin_y)
            first_change = (change[0][0] - drive * sheet[0], change[0][1] - drive * sheet[1])
            change = (first_change, change[1], change[2])
            electric = tuple(relax(couple, change_part, e_retain, e_factor) for couple, change_part in zip(electric, change))
            return (electric, magnetic)

        def snapshot(fields, index):
            fields = lax.fori_loop(0, INTERVAL, lambda inner, held: advance(held, waveform[index * INTERVAL + inner]), fields)
            electric = fields[0]
            power = (electric[0][0][:, :, monitor] ** 2 + electric[0][1][:, :, monitor] ** 2
                     + electric[1][0][:, :, monitor] ** 2 + electric[1][1][:, :, monitor] ** 2)
            return fields, jnp.sum(power) / power.size

        electric_wide = electric_begin.astype(jnp.float32)
        magnetic_wide = magnetic_begin.astype(jnp.float32)
        start_e = tuple((electric_wide[2 * member], electric_wide[2 * member + 1]) for member in range(3))
        start_h = tuple((magnetic_wide[2 * member], magnetic_wide[2 * member + 1]) for member in range(3))
        final, powers = lax.scan(snapshot, (start_e, start_h), jnp.arange(NSNAP))
        electric, magnetic = final
        electric_stack = jnp.stack([values for couple in electric for values in couple], 0)
        magnetic_stack = jnp.stack([values for couple in magnetic for values in couple], 0)
        return electric_stack, magnetic_stack, powers

    electric_out, magnetic_out, reflected = lax.map(one_point, (angles, source_sheet, electric_in, magnetic_in))
    reflected_mean = jnp.sum(reflected, 0) / reflected.shape[0]
    return electric_out, magnetic_out, reflected, reflected_mean
```

```python
import functools

import jax
import jax.numpy as jnp
from jax import lax
from jax.experimental import pallas as pl
from jax.experimental.pallas import tpu as pltpu
from jax.sharding import PartitionSpec as P

PML = 16
INTERVAL = 5
MPHASE = 64
NMAT = 3
TIME_STEP = 0.5
MESH = pl.DeviceIdType.MESH


def rotate(couple, cosine, sine):
    return (couple[0] * cosine - couple[1] * sine, couple[0] * sine + couple[1] * cosine)


def minus(left, right):
    return (left[0] - right[0], left[1] - right[1])


def plus(left, right):
    return (left[0] + right[0], left[1] + right[1])


def relax(couple, change, keep, gain):
    return tuple(keep * c + gain * d for c, d in zip(couple, change))


def kernel(
    bloch_ref,
    perm_ref,
    peak_ref,
    wave_ref,
    material_ref,
    sheet_ref,
    e_in,
    h_in,
    e_ref,
    h_ref,
    report_ref,
    keep_ref,
    gain_ref,
    drive_ref,
    out_e,
    out_w,
    got_e,
    got_w,
    send_e,
    send_w,
    recv_e,
    recv_w,
):
    rows, width, depth = material_ref.shape
    steps = wave_ref.shape[0]
    slabs = lax.axis_size("sp")
    slab = lax.axis_index("sp")
    upper = lax.rem(slab + 1, slabs)
    lower = lax.rem(slab + slabs - 1, slabs)

    barrier = pltpu.get_barrier_semaphore()
    for other in (lower, upper):
        pl.semaphore_signal(barrier, inc=1, device_id={"sp": other}, device_id_type=MESH)

    height = lax.broadcasted_iota(jnp.int32, (8, depth), 1).astype(jnp.float32)
    low_depth = jnp.maximum(PML - height, 0.0) / PML
    high_depth = jnp.maximum(height - (depth - 1 - PML), 0.0) / PML
    conduct = peak_ref[0] * (
        low_depth * low_depth * low_depth + high_depth * high_depth * high_depth
    )
    half_mag = conduct * (0.5 * TIME_STEP)
    h_keep = ((1.0 - half_mag) / (1.0 + half_mag))[0:1]
    h_gain = (-TIME_STEP / (1.0 + half_mag))[0:1]
    tables = []
    for level in range(NMAT):
        relative = jnp.full((8, depth), perm_ref[level], jnp.float32)
        half_ele = conduct * (0.5 * TIME_STEP) / relative
        tables.append(
            (
                ((1.0 - half_ele) / (1.0 + half_ele))[0:1],
                (TIME_STEP / relative / (1.0 + half_ele))[0:1],
            )
        )

    def trig(member):
        angle = jnp.full((8, depth), bloch_ref[0, member], jnp.int32).astype(jnp.float32)
        angle = 2.0 * jnp.pi * angle / MPHASE
        return jnp.cos(angle)[0:1], jnp.sin(angle)[0:1]

    cos_x, sin_x = trig(0)
    cos_y, sin_y = trig(1)
    at_end = (slab == slabs - 1).astype(jnp.float32)
    at_start = (slab == 0).astype(jnp.float32)
    end_cos = at_end * cos_x + (1.0 - at_end)
    end_sin = at_end * sin_x
    start_cos = at_start * cos_x + (1.0 - at_start)
    start_sin = -at_start * sin_x

    lane = lax.broadcasted_iota(jnp.int32, (width, depth), 1)
    last_lane = lane == depth - 1
    first_lane = lane == 0
    sub = lax.broadcasted_iota(jnp.int32, (8, depth), 0)

    def above_z(couple):
        return tuple(jnp.where(last_lane, 0.0, pltpu.roll(v, depth - 1, 1)) for v in couple)

    def below_z(couple):
        return tuple(jnp.where(first_lane, 0.0, pltpu.roll(v, 1, 1)) for v in couple)

    def above_y(couple):
        moved = tuple(pltpu.roll(v, width - 1, 0) for v in couple)
        tail = tuple(v[width - 8 :] for v in moved)
        turned = rotate(tail, cos_y, sin_y)
        return tuple(
            jnp.concatenate([v[: width - 8], jnp.where(sub == 7, r, w)], axis=0)
            for v, r, w in zip(moved, turned, tail)
        )

    def below_y(couple):
        moved = tuple(pltpu.roll(v, 1, 0) for v in couple)
        head = tuple(v[:8] for v in moved)
        turned = rotate(head, cos_y, -sin_y)
        return tuple(
            jnp.concatenate([jnp.where(sub == 0, r, w), v[8:]], axis=0)
            for v, r, w in zip(moved, turned, head)
        )

    def get(ref, member, x):
        return (ref[0, 2 * member, x], ref[0, 2 * member + 1, x])

    def put(ref, member, x, couple):
        ref[0, 2 * member, x] = couple[0]
        ref[0, 2 * member + 1, x] = couple[1]

    def get_plane(ref, slot, member):
        return (ref[slot, 2 * member], ref[slot, 2 * member + 1])

    def put_plane(ref, slot, member, couple):
        ref[slot, 2 * member] = couple[0]
        ref[slot, 2 * member + 1] = couple[1]

    def hx_plane(x):
        ey, ez = get(e_ref, 1, x), get(e_ref, 2, x)
        change = minus(minus(above_y(ez), ez), minus(above_z(ey), ey))
        put(h_ref, 0, x, relax(get(h_ref, 0, x), change, h_keep, h_gain))

    def h_plane(x, carry):
        hx_plane(x)
        ex, ey, ez = get(e_ref, 0, x), get(e_ref, 1, x), get(e_ref, 2, x)
        dx_ez = minus(get(e_ref, 2, x + 1), ez)
        dx_ey = minus(get(e_ref, 1, x + 1), ey)
        change = minus(minus(above_z(ex), ex), dx_ez)
        put(h_ref, 1, x, relax(get(h_ref, 1, x), change, h_keep, h_gain))
        change = minus(dx_ey, minus(above_y(ex), ex))
        put(h_ref, 2, x, relax(get(h_ref, 2, x), change, h_keep, h_gain))
        return carry

    def partial_h(slot):
        x = rows - 1
        ex, ey, ez = get(e_ref, 0, x), get(e_ref, 1, x), get(e_ref, 2, x)
        change = plus(minus(above_z(ex), ex), ez)
        put_plane(out_w, slot, 0, relax(get(h_ref, 1, x), change, h_keep, h_gain))
        change = minus(minus(ex, above_y(ex)), ey)
        put_plane(out_w, slot, 1, relax(get(h_ref, 2, x), change, h_keep, h_gain))

    def complete_h(slot):
        x = rows - 1
        beyond_y = rotate(get_plane(got_e, slot, 0), end_cos, end_sin)
        beyond_z = rotate(get_plane(got_e, slot, 1), end_cos, end_sin)
        w_y, w_z = get_plane(out_w, slot, 0), get_plane(out_w, slot, 1)
        put(h_ref, 1, x, tuple(w - h_gain * b for w, b in zip(w_y, beyond_z)))
        put(h_ref, 2, x, tuple(w + h_gain * b for w, b in zip(w_z, beyond_y)))

    def e_update(x, drive, hy_prev, hz_prev):
        hx, hy, hz = get(h_ref, 0, x), get(h_ref, 1, x), get(h_ref, 2, x)
        keep, gain = keep_ref[x], gain_ref[x]
        change = minus(minus(hz, below_y(hz)), minus(hy, below_z(hy)))
        change = (change[0] - drive * drive_ref[0, x], change[1] - drive * drive_ref[1, x])
        put(e_ref, 0, x, relax(get(e_ref, 0, x), change, keep, gain))
        change = minus(minus(hx, below_z(hx)), minus(hz, hz_prev))
        ey = relax(get(e_ref, 1, x), change, keep, gain)
        put(e_ref, 1, x, ey)
        change = minus(minus(hy, hy_prev), minus(hx, below_y(hx)))
        ez = relax(get(e_ref, 2, x), change, keep, gain)
        put(e_ref, 2, x, ez)
        return ey, ez

    def e_first(slot, drive):
        ey, ez = get(e_ref, 1, 0), get(e_ref, 2, 0)
        turned_y = rotate(get_plane(got_w, slot, 0), start_cos, start_sin)
        turned_z = rotate(get_plane(got_w, slot, 1), start_cos, start_sin)
        hy_prev = tuple(w - h_gain * e for w, e in zip(turned_y, ez))
        hz_prev = tuple(w + h_gain * e for w, e in zip(turned_z, ey))
        return e_update(0, drive, hy_prev, hz_prev)

    def copy_e(slot):
        return pltpu.make_async_remote_copy(
            src_ref=out_e.at[slot],
            dst_ref=got_e.at[slot],
            send_sem=send_e.at[slot],
            recv_sem=recv_e.at[slot],
            device_id={"sp": lower},
            device_id_type=MESH,
        )

    def copy_w(slot):
        return pltpu.make_async_remote_copy(
            src_ref=out_w.at[slot],
            dst_ref=got_w.at[slot],
            send_sem=send_w.at[slot],
            recv_sem=recv_w.at[slot],
            device_id={"sp": upper},
            device_id_type=MESH,
        )

    def widen(x, carry):
        for member in range(6):
            e_ref[0, member, x] = e_in[0, member, x].astype(jnp.float32)
            h_ref[0, member, x] = h_in[0, member, x].astype(jnp.float32)
        return carry

    widen(0, 0)
    widen(rows - 1, 0)
    for member in range(2):
        put_plane(out_e, 0, member, get(e_ref, 1 + member, 0))
    partial_h(0)
    pl.semaphore_wait(barrier, 2)
    copy_e(0).start()
    copy_w(0).start()
    lax.fori_loop(1, rows - 1, widen, 0)

    square = lax.broadcasted_iota(jnp.int32, (width, width), 0) == lax.broadcasted_iota(
        jnp.int32, (width, width), 1
    )

    def prepare(x, carry):
        kind = material_ref[x]
        keep, gain = tables[0]
        for level in range(1, NMAT):
            keep = jnp.where(kind == level, tables[level][0], keep)
            gain = jnp.where(kind == level, tables[level][1], gain)
        keep_ref[x] = keep
        gain_ref[x] = gain
        for part in range(2):
            row = sheet_ref[0, part, pl.ds(x, 1), :]
            column = jnp.sum(jnp.where(square, row, 0.0), axis=1, keepdims=True)
            drive_ref[part, x] = jnp.where(lane == PML + 2, column, 0.0)
        return carry

    lax.fori_loop(0, rows, prepare, 0)

    def step(t, carry):
        slot = lax.rem(t, 2)
        later = lax.rem(t + 1, 2)
        drive = wave_ref[t]
        lax.fori_loop(0, rows - 1, h_plane, 0)
        hx_plane(rows - 1)
        copy_w(slot).wait_recv()
        ey, ez = e_first(slot, drive)

        @pl.when(jnp.logical_and(t >= 1, t < steps - 1))
        def _():
            copy_e(later).wait_send()

        @pl.when(t < steps - 1)
        def _():
            put_plane(out_e, later, 0, ey)
            put_plane(out_e, later, 1, ez)
            copy_e(later).start()

        def inner(x, held):
            e_update(x, drive, get(h_ref, 1, x - 1), get(h_ref, 2, x - 1))
            return held

        lax.fori_loop(1, rows - 1, inner, 0)
        copy_e(slot).wait_recv()
        complete_h(slot)
        e_update(rows - 1, drive, get(h_ref, 1, rows - 2), get(h_ref, 2, rows - 2))

        @pl.when(jnp.logical_and(t >= 1, t < steps - 1))
        def _():
            copy_w(later).wait_send()

        @pl.when(t < steps - 1)
        def _():
            partial_h(later)
            copy_w(later).start()

        @pl.when(lax.rem(t + 1, INTERVAL) == 0)
        def _():
            def power(x, total):
                for member in range(4):
                    value = e_ref[0, member, x]
                    total = total + value * value
                return total

            total = lax.fori_loop(0, rows, power, jnp.zeros((width, depth), jnp.float32))
            folded = total[0:8]
            for at in range(8, width, 8):
                folded = folded + total[at : at + 8]
            report_ref[lax.div(t, INTERVAL)] = folded

        return carry

    lax.fori_loop(0, steps, step, 0)
    for t in (steps - 2, steps - 1):
        copy_e(t % 2).wait_send()
        copy_w(t % 2).wait_send()


def one_point(bloch, material, permittivity, peak, sheet, waveform, electric, magnetic):
    rows, width, depth = material.shape
    snaps = waveform.shape[0] // INTERVAL
    smem = pl.BlockSpec(memory_space=pltpu.SMEM)
    vmem = pl.BlockSpec(memory_space=pltpu.VMEM)
    plane = (2, 4, width, depth)
    f32 = jnp.float32
    return pl.pallas_call(
        kernel,
        out_shape=(
            jax.ShapeDtypeStruct(electric.shape, f32),
            jax.ShapeDtypeStruct(magnetic.shape, f32),
            jax.ShapeDtypeStruct((snaps, 8, depth), f32),
        ),
        in_specs=[smem] * 4 + [vmem] * 4,
        out_specs=(vmem, vmem, vmem),
        scratch_shapes=[
            pltpu.VMEM((rows, width, depth), f32),
            pltpu.VMEM((rows, width, depth), f32),
            pltpu.VMEM((2, rows, width, depth), f32),
            pltpu.VMEM(plane, f32),
            pltpu.VMEM(plane, f32),
            pltpu.VMEM(plane, f32),
            pltpu.VMEM(plane, f32),
            pltpu.SemaphoreType.DMA((2,)),
            pltpu.SemaphoreType.DMA((2,)),
            pltpu.SemaphoreType.DMA((2,)),
            pltpu.SemaphoreType.DMA((2,)),
        ],
        compiler_params=pltpu.CompilerParams(
            collective_id=0, has_side_effects=True, vmem_limit_bytes=40 * 1024 * 1024
        ),
    )(bloch, permittivity, peak, waveform, material, sheet, electric, magnetic)


def on_device(
    bloch_index,
    material,
    permittivity,
    absorption_peak,
    source_sheet,
    waveform,
    electric_in,
    magnetic_in,
):
    points = bloch_index.shape[0]
    rows, width, depth = material.shape
    slabs = lax.axis_size("sp")
    results = [
        one_point(
            bloch_index[p : p + 1],
            material,
            permittivity,
            absorption_peak,
            source_sheet[p : p + 1],
            waveform,
            electric_in[p : p + 1],
            magnetic_in[p : p + 1],
        )
        for p in range(points)
    ]
    electric_out = jnp.concatenate([r[0] for r in results], 0)
    magnetic_out = jnp.concatenate([r[1] for r in results], 0)
    reports = jnp.stack([jnp.sum(r[2][:, :, PML + 6], axis=1) for r in results], 0)
    reflected = lax.psum(reports / (rows * slabs * width), "sp")
    total_points = points * lax.axis_size("ka")
    reflected_mean = lax.psum(jnp.sum(reflected, 0) / total_points, "ka")
    return (electric_out, magnetic_out, reflected, reflected_mean)


def solution(mesh):
    in_specs = (
        P("ka", None),
        P("sp", None, None),
        P(),
        P(),
        P("ka", None, "sp", None),
        P(),
        P("ka", None, "sp", None, None),
        P("ka", None, "sp", None, None),
    )
    out_specs = (
        P("ka", None, "sp", None, None),
        P("ka", None, "sp", None, None),
        P("ka", None),
        P(),
    )
    return jax.shard_map(
        on_device, mesh=mesh, in_specs=in_specs, out_specs=out_specs, check_vma=False
    )
```

```python
import jax
import jax.numpy as jnp
from jax import lax
from jax.experimental import pallas as pl
from jax.experimental.pallas import tpu as pltpu
from jax.sharding import PartitionSpec as P

PML = 16
INTERVAL = 5
MPHASE = 64
NMAT = 3
TIME_STEP = 0.5
MESH = pl.DeviceIdType.MESH


def rotate(couple, cosine, sine):
    return (couple[0] * cosine - couple[1] * sine, couple[0] * sine + couple[1] * cosine)


def minus(left, right):
    return (left[0] - right[0], left[1] - right[1])


def plus(left, right):
    return (left[0] + right[0], left[1] + right[1])


def relax(couple, change, keep, gain):
    return tuple(keep * c + gain * d for c, d in zip(couple, change))


def kernel(
    bloch_in,
    perm_in,
    peak_in,
    wave_in,
    material_in,
    sheet_in,
    e_hbm,
    h_hbm,
    e_ref,
    h_ref,
    reflected_ref,
    mean_ref,
    bloch_ref,
    perm_ref,
    peak_ref,
    wave_ref,
    material_ref,
    sheet_ref,
    e_in,
    h_in,
    report_ref,
    got_report,
    keep_ref,
    gain_ref,
    drive_ref,
    out_e,
    out_w,
    got_e,
    got_w,
    send_e,
    send_w,
    recv_e,
    recv_w,
    load_sem,
    send_report,
    recv_report,
):
    rows, width, depth = material_ref.shape
    steps = wave_ref.shape[0]
    slabs = lax.axis_size("sp")
    slab = lax.axis_index("sp")
    upper = lax.rem(slab + 1, slabs)
    lower = lax.rem(slab + slabs - 1, slabs)

    groups = lax.axis_size("ka")
    group = lax.axis_index("ka")
    everyone = groups * slabs
    me = group * slabs + slab

    def place(at):
        return {"ka": lax.div(at, slabs), "sp": lax.rem(at, slabs)}

    last_row = rows - 1
    loads = [
        pltpu.make_async_copy(src, dst, load_sem.at[at])
        for at, (src, dst) in enumerate(
            (
                (e_hbm.at[0, :, last_row], e_in.at[0, :, last_row]),
                (h_hbm.at[0, :, last_row], h_in.at[0, :, last_row]),
                (e_hbm.at[0, :, 0], e_in.at[0, :, 0]),
                (h_hbm.at[0, :, 0], h_in.at[0, :, 0]),
                (bloch_in, bloch_ref),
                (perm_in, perm_ref),
                (peak_in, peak_ref),
                (wave_in, wave_ref),
                (e_hbm.at[0, :, 1:last_row], e_in.at[0, :, 1:last_row]),
                (h_hbm.at[0, :, 1:last_row], h_in.at[0, :, 1:last_row]),
                (material_in, material_ref),
                (sheet_in, sheet_ref),
            )
        )
    ]
    for load in loads:
        load.start()

    barrier = pltpu.get_barrier_semaphore()

    def greet(offset, carry):
        other = lax.rem(me + offset, everyone)
        pl.semaphore_signal(barrier, inc=1, device_id=place(other), device_id_type=MESH)
        return carry

    lax.fori_loop(1, everyone, greet, 0)
    for load in loads[4:8]:
        load.wait()

    height = lax.broadcasted_iota(jnp.int32, (8, depth), 1).astype(jnp.float32)
    low_depth = jnp.maximum(PML - height, 0.0) / PML
    high_depth = jnp.maximum(height - (depth - 1 - PML), 0.0) / PML
    conduct = peak_ref[0] * (
        low_depth * low_depth * low_depth + high_depth * high_depth * high_depth
    )
    half_mag = conduct * (0.5 * TIME_STEP)
    h_keep = ((1.0 - half_mag) / (1.0 + half_mag))[0:1]
    h_gain = (-TIME_STEP / (1.0 + half_mag))[0:1]
    tables = []
    for level in range(NMAT):
        relative = jnp.full((8, depth), perm_ref[level], jnp.float32)
        half_ele = conduct * (0.5 * TIME_STEP) / relative
        tables.append(
            (
                ((1.0 - half_ele) / (1.0 + half_ele))[0:1],
                (TIME_STEP / relative / (1.0 + half_ele))[0:1],
            )
        )

    def trig(member):
        angle = jnp.full((8, depth), bloch_ref[0, member], jnp.int32).astype(jnp.float32)
        angle = 2.0 * jnp.pi * angle / MPHASE
        return jnp.cos(angle)[0:1], jnp.sin(angle)[0:1]

    cos_x, sin_x = trig(0)
    cos_y, sin_y = trig(1)
    at_end = (slab == slabs - 1).astype(jnp.float32)
    at_start = (slab == 0).astype(jnp.float32)
    end_cos = at_end * cos_x + (1.0 - at_end)
    end_sin = at_end * sin_x
    start_cos = at_start * cos_x + (1.0 - at_start)
    start_sin = -at_start * sin_x

    lane = lax.broadcasted_iota(jnp.int32, (width, depth), 1)
    last_lane = lane == depth - 1
    first_lane = lane == 0
    sub = lax.broadcasted_iota(jnp.int32, (8, depth), 0)

    def above_z(couple):
        return tuple(jnp.where(last_lane, 0.0, pltpu.roll(v, depth - 1, 1)) for v in couple)

    def below_z(couple):
        return tuple(jnp.where(first_lane, 0.0, pltpu.roll(v, 1, 1)) for v in couple)

    def above_y(couple):
        moved = tuple(pltpu.roll(v, width - 1, 0) for v in couple)
        tail = tuple(v[width - 8 :] for v in moved)
        turned = rotate(tail, cos_y, sin_y)
        return tuple(
            jnp.concatenate([v[: width - 8], jnp.where(sub == 7, r, w)], axis=0)
            for v, r, w in zip(moved, turned, tail)
        )

    def below_y(couple):
        moved = tuple(pltpu.roll(v, 1, 0) for v in couple)
        head = tuple(v[:8] for v in moved)
        turned = rotate(head, cos_y, -sin_y)
        return tuple(
            jnp.concatenate([jnp.where(sub == 0, r, w), v[8:]], axis=0)
            for v, r, w in zip(moved, turned, head)
        )

    def get(ref, member, x):
        return (ref[0, 2 * member, x], ref[0, 2 * member + 1, x])

    def put(ref, member, x, couple):
        ref[0, 2 * member, x] = couple[0]
        ref[0, 2 * member + 1, x] = couple[1]

    def get_plane(ref, slot, member):
        return (ref[slot, 2 * member], ref[slot, 2 * member + 1])

    def put_plane(ref, slot, member, couple):
        ref[slot, 2 * member] = couple[0]
        ref[slot, 2 * member + 1] = couple[1]

    def hx_plane(x):
        ey, ez = get(e_ref, 1, x), get(e_ref, 2, x)
        change = minus(minus(above_y(ez), ez), minus(above_z(ey), ey))
        put(h_ref, 0, x, relax(get(h_ref, 0, x), change, h_keep, h_gain))

    def h_plane(x, carry):
        hx_plane(x)
        ex, ey, ez = get(e_ref, 0, x), get(e_ref, 1, x), get(e_ref, 2, x)
        dx_ez = minus(get(e_ref, 2, x + 1), ez)
        dx_ey = minus(get(e_ref, 1, x + 1), ey)
        change = minus(minus(above_z(ex), ex), dx_ez)
        put(h_ref, 1, x, relax(get(h_ref, 1, x), change, h_keep, h_gain))
        change = minus(dx_ey, minus(above_y(ex), ex))
        put(h_ref, 2, x, relax(get(h_ref, 2, x), change, h_keep, h_gain))
        return carry

    def partial_h(slot):
        x = rows - 1
        ex, ey, ez = get(e_ref, 0, x), get(e_ref, 1, x), get(e_ref, 2, x)
        change = plus(minus(above_z(ex), ex), ez)
        put_plane(out_w, slot, 0, relax(get(h_ref, 1, x), change, h_keep, h_gain))
        change = minus(minus(ex, above_y(ex)), ey)
        put_plane(out_w, slot, 1, relax(get(h_ref, 2, x), change, h_keep, h_gain))

    def complete_h(slot):
        x = rows - 1
        beyond_y = rotate(get_plane(got_e, slot, 0), end_cos, end_sin)
        beyond_z = rotate(get_plane(got_e, slot, 1), end_cos, end_sin)
        w_y, w_z = get_plane(out_w, slot, 0), get_plane(out_w, slot, 1)
        put(h_ref, 1, x, tuple(w - h_gain * b for w, b in zip(w_y, beyond_z)))
        put(h_ref, 2, x, tuple(w + h_gain * b for w, b in zip(w_z, beyond_y)))

    def e_update(x, drive, hy_prev, hz_prev):
        hx, hy, hz = get(h_ref, 0, x), get(h_ref, 1, x), get(h_ref, 2, x)
        keep, gain = keep_ref[x], gain_ref[x]
        change = minus(minus(hz, below_y(hz)), minus(hy, below_z(hy)))
        change = (change[0] - drive * drive_ref[0, x], change[1] - drive * drive_ref[1, x])
        put(e_ref, 0, x, relax(get(e_ref, 0, x), change, keep, gain))
        change = minus(minus(hx, below_z(hx)), minus(hz, hz_prev))
        ey = relax(get(e_ref, 1, x), change, keep, gain)
        put(e_ref, 1, x, ey)
        change = minus(minus(hy, hy_prev), minus(hx, below_y(hx)))
        ez = relax(get(e_ref, 2, x), change, keep, gain)
        put(e_ref, 2, x, ez)
        return ey, ez

    def e_first(slot, drive):
        ey, ez = get(e_ref, 1, 0), get(e_ref, 2, 0)
        turned_y = rotate(get_plane(got_w, slot, 0), start_cos, start_sin)
        turned_z = rotate(get_plane(got_w, slot, 1), start_cos, start_sin)
        hy_prev = tuple(w - h_gain * e for w, e in zip(turned_y, ez))
        hz_prev = tuple(w + h_gain * e for w, e in zip(turned_z, ey))
        return e_update(0, drive, hy_prev, hz_prev)

    def copy_e(slot):
        return pltpu.make_async_remote_copy(
            src_ref=out_e.at[slot],
            dst_ref=got_e.at[slot],
            send_sem=send_e.at[slot],
            recv_sem=recv_e.at[slot],
            device_id={"sp": lower},
            device_id_type=MESH,
        )

    def copy_w(slot):
        return pltpu.make_async_remote_copy(
            src_ref=out_w.at[slot],
            dst_ref=got_w.at[slot],
            send_sem=send_w.at[slot],
            recv_sem=recv_w.at[slot],
            device_id={"sp": upper},
            device_id_type=MESH,
        )

    def widen(x, carry):
        for member in range(6):
            e_ref[0, member, x] = e_in[0, member, x].astype(jnp.float32)
            h_ref[0, member, x] = h_in[0, member, x].astype(jnp.float32)
        return carry

    for load in loads[0:4]:
        load.wait()
    widen(rows - 1, 0)
    partial_h(0)
    widen(0, 0)
    for member in range(2):
        put_plane(out_e, 0, member, get(e_ref, 1 + member, 0))
    pl.semaphore_wait(barrier, everyone - 1)
    copy_w(0).start()
    copy_e(0).start()
    for load in loads[8:]:
        load.wait()
    lax.fori_loop(1, rows - 1, widen, 0)

    report_ref[...] = jnp.zeros_like(report_ref)
    square = lax.broadcasted_iota(jnp.int32, (width, width), 0) == lax.broadcasted_iota(
        jnp.int32, (width, width), 1
    )

    def prepare(x, carry):
        kind = material_ref[x]
        keep, gain = tables[0]
        for level in range(1, NMAT):
            keep = jnp.where(kind == level, tables[level][0], keep)
            gain = jnp.where(kind == level, tables[level][1], gain)
        keep_ref[x] = keep
        gain_ref[x] = gain
        for part in range(2):
            row = sheet_ref[0, part, pl.ds(x, 1), :]
            column = jnp.sum(jnp.where(square, row, 0.0), axis=1, keepdims=True)
            drive_ref[part, x] = jnp.where(lane == PML + 2, column, 0.0)
        return carry

    lax.fori_loop(0, rows, prepare, 0)

    def power(x, total):
        for member in range(4):
            value = e_ref[0, member, x]
            total = total + value * value
        return total

    def step(t, carry):
        slot = lax.rem(t, 2)
        later = lax.rem(t + 1, 2)
        drive = wave_ref[t]
        lax.fori_loop(0, rows - 1, h_plane, 0)
        hx_plane(rows - 1)
        copy_w(slot).wait_recv()
        ey, ez = e_first(slot, drive)

        @pl.when(jnp.logical_and(t >= 1, t < steps - 1))
        def _():
            copy_e(later).wait_send()

        @pl.when(t < steps - 1)
        def _():
            put_plane(out_e, later, 0, ey)
            put_plane(out_e, later, 1, ez)
            copy_e(later).start()

        def inner(x, held):
            e_update(x, drive, get(h_ref, 1, x - 1), get(h_ref, 2, x - 1))
            return held

        lax.fori_loop(1, rows - 1, inner, 0)

        @pl.when(lax.rem(t + 1, INTERVAL) == 0)
        def _():
            total = lax.fori_loop(0, rows - 1, power, jnp.zeros((width, depth), jnp.float32))
            report_ref[pl.ds(lax.div(t, INTERVAL), 1)] = jnp.sum(total, axis=0, keepdims=True)

        copy_e(slot).wait_recv()
        complete_h(slot)
        e_update(rows - 1, drive, get(h_ref, 1, rows - 2), get(h_ref, 2, rows - 2))

        @pl.when(jnp.logical_and(t >= 1, t < steps - 1))
        def _():
            copy_w(later).wait_send()

        @pl.when(t < steps - 1)
        def _():
            partial_h(later)
            copy_w(later).start()

        @pl.when(lax.rem(t + 1, INTERVAL) == 0)
        def _():
            total = power(rows - 1, jnp.zeros((width, depth), jnp.float32))
            at = lax.div(t, INTERVAL)
            report_ref[pl.ds(at, 1)] += jnp.sum(total, axis=0, keepdims=True)

        return carry

    lax.fori_loop(0, steps, step, 0)

    def tell(offset):
        return pltpu.make_async_remote_copy(
            src_ref=report_ref,
            dst_ref=got_report.at[me],
            send_sem=send_report,
            recv_sem=recv_report,
            device_id=place(lax.rem(me + offset, everyone)),
            device_id_type=MESH,
        )

    def tell_start(offset, carry):
        tell(offset).start()
        return carry

    lax.fori_loop(1, everyone, tell_start, 0)
    got_report[me] = report_ref[...]
    for t in (steps - 2, steps - 1):
        copy_e(t % 2).wait_send()
        copy_w(t % 2).wait_send()
    everything = got_report.at[pl.ds(0, everyone - 1)]
    pltpu.make_async_copy(everything, everything, recv_report).wait()
    pltpu.make_async_copy(everything, everything, send_report).wait()

    def gather(at, held):
        value = got_report[at]
        ours = (lax.div(at, slabs) == group).astype(jnp.float32)
        return held[0] + value, held[1] + ours * value

    zero = jnp.zeros(report_ref.shape, jnp.float32)
    total, ours = lax.fori_loop(0, everyone, gather, (zero, zero))
    cells = rows * slabs * width
    reflected_ref[...] = ours / cells
    mean_ref[...] = total / cells / groups


def one_point(bloch, material, permittivity, peak, sheet, waveform, electric, magnetic):
    rows, width, depth = material.shape
    snaps = waveform.shape[0] // INTERVAL
    everyone = lax.axis_size("ka") * lax.axis_size("sp")
    hbm = pl.BlockSpec(memory_space=pltpu.HBM)
    lines = -(-snaps // 8) * 8
    vmem = pl.BlockSpec(memory_space=pltpu.VMEM)
    plane = (2, 4, width, depth)
    f32 = jnp.float32
    return pl.pallas_call(
        kernel,
        out_shape=(
            jax.ShapeDtypeStruct(electric.shape, f32),
            jax.ShapeDtypeStruct(magnetic.shape, f32),
            jax.ShapeDtypeStruct((lines, depth), f32),
            jax.ShapeDtypeStruct((lines, depth), f32),
        ),
        in_specs=[hbm] * 8,
        out_specs=(vmem, vmem, vmem, vmem),
        scratch_shapes=[
            pltpu.SMEM(bloch.shape, jnp.int32),
            pltpu.SMEM(permittivity.shape, f32),
            pltpu.SMEM(peak.shape, f32),
            pltpu.SMEM(waveform.shape, f32),
            pltpu.VMEM(material.shape, jnp.int32),
            pltpu.VMEM(sheet.shape, f32),
            pltpu.VMEM(electric.shape, electric.dtype),
            pltpu.VMEM(magnetic.shape, magnetic.dtype),
            pltpu.VMEM((lines, depth), f32),
            pltpu.VMEM((everyone, lines, depth), f32),
            pltpu.VMEM((rows, width, depth), f32),
            pltpu.VMEM((rows, width, depth), f32),
            pltpu.VMEM((2, rows, width, depth), f32),
            pltpu.VMEM(plane, f32),
            pltpu.VMEM(plane, f32),
            pltpu.VMEM(plane, f32),
            pltpu.VMEM(plane, f32),
            pltpu.SemaphoreType.DMA((2,)),
            pltpu.SemaphoreType.DMA((2,)),
            pltpu.SemaphoreType.DMA((2,)),
            pltpu.SemaphoreType.DMA((2,)),
            pltpu.SemaphoreType.DMA((12,)),
            pltpu.SemaphoreType.DMA,
            pltpu.SemaphoreType.DMA,
        ],
        compiler_params=pltpu.CompilerParams(
            collective_id=0, has_side_effects=True, vmem_limit_bytes=40 * 1024 * 1024
        ),
    )(bloch, permittivity, peak, waveform, material, sheet, electric, magnetic)


def on_device(
    bloch_index,
    material,
    permittivity,
    absorption_peak,
    source_sheet,
    waveform,
    electric_in,
    magnetic_in,
):
    points = bloch_index.shape[0]
    results = [
        one_point(
            bloch_index[p : p + 1],
            material,
            permittivity,
            absorption_peak,
            source_sheet[p : p + 1],
            waveform,
            electric_in[p : p + 1],
            magnetic_in[p : p + 1],
        )
        for p in range(points)
    ]
    electric_out = jnp.concatenate([r[0] for r in results], 0)
    magnetic_out = jnp.concatenate([r[1] for r in results], 0)
    snaps = waveform.shape[0] // INTERVAL
    reflected = jnp.stack([r[2][:snaps, PML + 6] for r in results], 0)
    reflected_mean = sum(r[3][:snaps, PML + 6] for r in results) / points
    return (electric_out, magnetic_out, reflected, reflected_mean)


def solution(mesh):
    in_specs = (
        P("ka", None),
        P("sp", None, None),
        P(),
        P(),
        P("ka", None, "sp", None),
        P(),
        P("ka", None, "sp", None, None),
        P("ka", None, "sp", None, None),
    )
    out_specs = (
        P("ka", None, "sp", None, None),
        P("ka", None, "sp", None, None),
        P("ka", None),
        P(),
    )
    return jax.shard_map(
        on_device, mesh=mesh, in_specs=in_specs, out_specs=out_specs, check_vma=False
    )
```

```python
import jax
import jax.numpy as jnp
from jax import lax
from jax.experimental import pallas as pl
from jax.experimental.pallas import tpu as pltpu
from jax.sharding import PartitionSpec as P

PML = 16
INTERVAL = 5
MPHASE = 64
NMAT = 3
TIME_STEP = 0.5
MESH = pl.DeviceIdType.MESH


def rotate(couple, cosine, sine):
    return (couple[0] * cosine - couple[1] * sine, couple[0] * sine + couple[1] * cosine)


def minus(left, right):
    return (left[0] - right[0], left[1] - right[1])


def plus(left, right):
    return (left[0] + right[0], left[1] + right[1])


def relax(couple, change, keep, gain):
    return tuple(keep * c + gain * d for c, d in zip(couple, change))


def kernel(
    bloch_in,
    perm_in,
    peak_in,
    wave_in,
    material_in,
    sheet_in,
    e_hbm,
    h_hbm,
    e_ref,
    h_ref,
    reflected_ref,
    mean_ref,
    bloch_ref,
    perm_ref,
    peak_ref,
    wave_ref,
    material_ref,
    sheet_ref,
    e_in,
    h_in,
    report_ref,
    got_report,
    keep_ref,
    gain_ref,
    drive_ref,
    out_e,
    out_w,
    got_e,
    got_w,
    send_e,
    send_w,
    recv_e,
    recv_w,
    load_sem,
    send_report,
    recv_report,
):
    rows, width, depth = material_ref.shape
    steps = wave_ref.shape[0]
    slabs = lax.axis_size("sp")
    slab = lax.axis_index("sp")
    upper = lax.rem(slab + 1, slabs)
    lower = lax.rem(slab + slabs - 1, slabs)

    groups = lax.axis_size("ka")
    group = lax.axis_index("ka")
    everyone = groups * slabs
    me = group * slabs + slab

    def place(at):
        return {"ka": lax.div(at, slabs), "sp": lax.rem(at, slabs)}

    last_row = rows - 1
    loads = [
        pltpu.make_async_copy(src, dst, load_sem.at[at])
        for at, (src, dst) in enumerate(
            (
                (e_hbm.at[0, :, last_row], e_in.at[0, :, last_row]),
                (h_hbm.at[0, :, last_row], h_in.at[0, :, last_row]),
                (e_hbm.at[0, :, 0], e_in.at[0, :, 0]),
                (h_hbm.at[0, :, 0], h_in.at[0, :, 0]),
                (bloch_in, bloch_ref),
                (perm_in, perm_ref),
                (peak_in, peak_ref),
                (wave_in, wave_ref),
                (e_hbm.at[0, :, 1:last_row], e_in.at[0, :, 1:last_row]),
                (h_hbm.at[0, :, 1:last_row], h_in.at[0, :, 1:last_row]),
                (material_in, material_ref),
                (sheet_in, sheet_ref),
            )
        )
    ]
    for load in loads:
        load.start()

    barrier = pltpu.get_barrier_semaphore()

    def greet(offset, carry):
        other = lax.rem(me + offset, everyone)
        pl.semaphore_signal(barrier, inc=1, device_id=place(other), device_id_type=MESH)
        return carry

    lax.fori_loop(1, everyone, greet, 0)
    for load in loads[4:8]:
        load.wait()

    height = lax.broadcasted_iota(jnp.int32, (8, depth), 1).astype(jnp.float32)
    low_depth = jnp.maximum(PML - height, 0.0) / PML
    high_depth = jnp.maximum(height - (depth - 1 - PML), 0.0) / PML
    conduct = peak_ref[0] * (
        low_depth * low_depth * low_depth + high_depth * high_depth * high_depth
    )
    half_mag = conduct * (0.5 * TIME_STEP)
    h_keep = ((1.0 - half_mag) / (1.0 + half_mag))[0:1]
    h_gain = (-TIME_STEP / (1.0 + half_mag))[0:1]
    tables = []
    for level in range(NMAT):
        relative = jnp.full((8, depth), perm_ref[level], jnp.float32)
        half_ele = conduct * (0.5 * TIME_STEP) / relative
        tables.append(
            (
                ((1.0 - half_ele) / (1.0 + half_ele))[0:1],
                (TIME_STEP / relative / (1.0 + half_ele))[0:1],
            )
        )

    def trig(member):
        angle = jnp.full((8, depth), bloch_ref[0, member], jnp.int32).astype(jnp.float32)
        angle = 2.0 * jnp.pi * angle / MPHASE
        return jnp.cos(angle)[0:1], jnp.sin(angle)[0:1]

    cos_x, sin_x = trig(0)
    cos_y, sin_y = trig(1)
    at_end = (slab == slabs - 1).astype(jnp.float32)
    at_start = (slab == 0).astype(jnp.float32)
    end_cos = at_end * cos_x + (1.0 - at_end)
    end_sin = at_end * sin_x
    start_cos = at_start * cos_x + (1.0 - at_start)
    start_sin = -at_start * sin_x

    lane = lax.broadcasted_iota(jnp.int32, (width, depth), 1)
    last_lane = lane == depth - 1
    first_lane = lane == 0
    sub = lax.broadcasted_iota(jnp.int32, (8, depth), 0)

    def above_z(couple):
        return tuple(jnp.where(last_lane, 0.0, pltpu.roll(v, depth - 1, 1)) for v in couple)

    def below_z(couple):
        return tuple(jnp.where(first_lane, 0.0, pltpu.roll(v, 1, 1)) for v in couple)

    def above_y(couple):
        moved = tuple(pltpu.roll(v, width - 1, 0) for v in couple)
        tail = tuple(v[width - 8 :] for v in moved)
        turned = rotate(tail, cos_y, sin_y)
        return tuple(
            jnp.concatenate([v[: width - 8], jnp.where(sub == 7, r, w)], axis=0)
            for v, r, w in zip(moved, turned, tail)
        )

    def below_y(couple):
        moved = tuple(pltpu.roll(v, 1, 0) for v in couple)
        head = tuple(v[:8] for v in moved)
        turned = rotate(head, cos_y, -sin_y)
        return tuple(
            jnp.concatenate([jnp.where(sub == 0, r, w), v[8:]], axis=0)
            for v, r, w in zip(moved, turned, head)
        )

    def get(ref, member, x):
        return (ref[0, 2 * member, x], ref[0, 2 * member + 1, x])

    def put(ref, member, x, couple):
        ref[0, 2 * member, x] = couple[0]
        ref[0, 2 * member + 1, x] = couple[1]

    def get_plane(ref, slot, member):
        return (ref[slot, 2 * member], ref[slot, 2 * member + 1])

    def put_plane(ref, slot, member, couple):
        ref[slot, 2 * member] = couple[0]
        ref[slot, 2 * member + 1] = couple[1]

    def hx_plane(x):
        ey, ez = get(e_ref, 1, x), get(e_ref, 2, x)
        change = minus(minus(above_y(ez), ez), minus(above_z(ey), ey))
        put(h_ref, 0, x, relax(get(h_ref, 0, x), change, h_keep, h_gain))

    def h_plane(x, carry):
        hx_plane(x)
        ex, ey, ez = get(e_ref, 0, x), get(e_ref, 1, x), get(e_ref, 2, x)
        dx_ez = minus(get(e_ref, 2, x + 1), ez)
        dx_ey = minus(get(e_ref, 1, x + 1), ey)
        change = minus(minus(above_z(ex), ex), dx_ez)
        put(h_ref, 1, x, relax(get(h_ref, 1, x), change, h_keep, h_gain))
        change = minus(dx_ey, minus(above_y(ex), ex))
        put(h_ref, 2, x, relax(get(h_ref, 2, x), change, h_keep, h_gain))
        return carry

    def partial_h(slot):
        x = rows - 1
        ex, ey, ez = get(e_ref, 0, x), get(e_ref, 1, x), get(e_ref, 2, x)
        change = plus(minus(above_z(ex), ex), ez)
        put_plane(out_w, slot, 0, relax(get(h_ref, 1, x), change, h_keep, h_gain))
        change = minus(minus(ex, above_y(ex)), ey)
        put_plane(out_w, slot, 1, relax(get(h_ref, 2, x), change, h_keep, h_gain))

    def complete_h(slot):
        x = rows - 1
        beyond_y = rotate(get_plane(got_e, slot, 0), end_cos, end_sin)
        beyond_z = rotate(get_plane(got_e, slot, 1), end_cos, end_sin)
        w_y, w_z = get_plane(out_w, slot, 0), get_plane(out_w, slot, 1)
        put(h_ref, 1, x, tuple(w - h_gain * b for w, b in zip(w_y, beyond_z)))
        put(h_ref, 2, x, tuple(w + h_gain * b for w, b in zip(w_z, beyond_y)))

    def e_update(x, drive, hy_prev, hz_prev):
        hx, hy, hz = get(h_ref, 0, x), get(h_ref, 1, x), get(h_ref, 2, x)
        keep, gain = keep_ref[x], gain_ref[x]
        change = minus(minus(hz, below_y(hz)), minus(hy, below_z(hy)))
        change = (change[0] - drive * drive_ref[0, x], change[1] - drive * drive_ref[1, x])
        put(e_ref, 0, x, relax(get(e_ref, 0, x), change, keep, gain))
        change = minus(minus(hx, below_z(hx)), minus(hz, hz_prev))
        ey = relax(get(e_ref, 1, x), change, keep, gain)
        put(e_ref, 1, x, ey)
        change = minus(minus(hy, hy_prev), minus(hx, below_y(hx)))
        ez = relax(get(e_ref, 2, x), change, keep, gain)
        put(e_ref, 2, x, ez)
        return ey, ez

    def e_first(slot, drive):
        ey, ez = get(e_ref, 1, 0), get(e_ref, 2, 0)
        turned_y = rotate(get_plane(got_w, slot, 0), start_cos, start_sin)
        turned_z = rotate(get_plane(got_w, slot, 1), start_cos, start_sin)
        hy_prev = tuple(w - h_gain * e for w, e in zip(turned_y, ez))
        hz_prev = tuple(w + h_gain * e for w, e in zip(turned_z, ey))
        return e_update(0, drive, hy_prev, hz_prev)

    def copy_e(slot):
        return pltpu.make_async_remote_copy(
            src_ref=out_e.at[slot],
            dst_ref=got_e.at[slot],
            send_sem=send_e.at[slot],
            recv_sem=recv_e.at[slot],
            device_id={"sp": lower},
            device_id_type=MESH,
        )

    def copy_w(slot):
        return pltpu.make_async_remote_copy(
            src_ref=out_w.at[slot],
            dst_ref=got_w.at[slot],
            send_sem=send_w.at[slot],
            recv_sem=recv_w.at[slot],
            device_id={"sp": upper},
            device_id_type=MESH,
        )

    def widen(x, carry):
        for member in range(6):
            e_ref[0, member, x] = e_in[0, member, x].astype(jnp.float32)
            h_ref[0, member, x] = h_in[0, member, x].astype(jnp.float32)
        return carry

    for load in loads[0:4]:
        load.wait()
    widen(rows - 1, 0)
    partial_h(0)
    widen(0, 0)
    for member in range(2):
        put_plane(out_e, 0, member, get(e_ref, 1 + member, 0))
    pl.semaphore_wait(barrier, everyone - 1)
    copy_w(0).start()
    copy_e(0).start()
    for load in loads[8:]:
        load.wait()
    lax.fori_loop(1, rows - 1, widen, 0)

    report_ref[...] = jnp.zeros_like(report_ref)
    square = lax.broadcasted_iota(jnp.int32, (width, width), 0) == lax.broadcasted_iota(
        jnp.int32, (width, width), 1
    )

    def prepare(x, carry):
        kind = material_ref[x]
        keep, gain = tables[0]
        for level in range(1, NMAT):
            keep = jnp.where(kind == level, tables[level][0], keep)
            gain = jnp.where(kind == level, tables[level][1], gain)
        keep_ref[x] = keep
        gain_ref[x] = gain
        for part in range(2):
            row = sheet_ref[0, part, pl.ds(x, 1), :]
            column = jnp.sum(jnp.where(square, row, 0.0), axis=1, keepdims=True)
            drive_ref[part, x] = jnp.where(lane == PML + 2, column, 0.0)
        return carry

    lax.fori_loop(0, rows, prepare, 0)

    def power(x, total):
        for member in range(4):
            value = e_ref[0, member, x]
            total = total + value * value
        return total

    def step(t, carry):
        slot = lax.rem(t, 2)
        later = lax.rem(t + 1, 2)
        drive = wave_ref[t]
        even = slot == 0
        ready = jnp.logical_and(t >= 1, t < steps - 1)
        snapshot = lax.rem(t + 1, INTERVAL) == 0
        empty = jnp.zeros((width, depth), jnp.float32)

        def left():
            copy_w(slot).wait_recv()
            ey, ez = e_first(slot, drive)

            @pl.when(ready)
            def _():
                copy_e(later).wait_send()

            @pl.when(t < steps - 1)
            def _():
                put_plane(out_e, later, 0, ey)
                put_plane(out_e, later, 1, ez)
                copy_e(later).start()

        def right():
            copy_e(slot).wait_recv()
            complete_h(slot)
            e_update(rows - 1, drive, get(h_ref, 1, rows - 2), get(h_ref, 2, rows - 2))

            @pl.when(ready)
            def _():
                copy_w(later).wait_send()

            @pl.when(t < steps - 1)
            def _():
                partial_h(later)
                copy_w(later).start()

        def inner(x, held):
            e_update(x, drive, get(h_ref, 1, x - 1), get(h_ref, 2, x - 1))
            return held

        lax.fori_loop(0, rows - 1, h_plane, 0)
        hx_plane(rows - 1)
        pl.when(even)(left)
        pl.when(jnp.logical_not(even))(right)
        lax.fori_loop(1, rows - 1, inner, 0)

        @pl.when(snapshot)
        def _():
            total = lax.fori_loop(1, rows - 1, power, empty)
            report_ref[pl.ds(lax.div(t, INTERVAL), 1)] = jnp.sum(total, axis=0, keepdims=True)

        pl.when(even)(right)
        pl.when(jnp.logical_not(even))(left)

        @pl.when(snapshot)
        def _():
            total = power(0, power(rows - 1, empty))
            at = lax.div(t, INTERVAL)
            report_ref[pl.ds(at, 1)] += jnp.sum(total, axis=0, keepdims=True)

        return carry

    lax.fori_loop(0, steps, step, 0)

    def tell(offset):
        return pltpu.make_async_remote_copy(
            src_ref=report_ref,
            dst_ref=got_report.at[me],
            send_sem=send_report,
            recv_sem=recv_report,
            device_id=place(lax.rem(me + offset, everyone)),
            device_id_type=MESH,
        )

    def tell_start(offset, carry):
        tell(offset).start()
        return carry

    lax.fori_loop(1, everyone, tell_start, 0)
    got_report[me] = report_ref[...]
    for t in (steps - 2, steps - 1):
        copy_e(t % 2).wait_send()
        copy_w(t % 2).wait_send()
    everything = got_report.at[pl.ds(0, everyone - 1)]
    pltpu.make_async_copy(everything, everything, recv_report).wait()
    pltpu.make_async_copy(everything, everything, send_report).wait()

    def gather(at, held):
        value = got_report[at]
        ours = (lax.div(at, slabs) == group).astype(jnp.float32)
        return held[0] + value, held[1] + ours * value

    zero = jnp.zeros(report_ref.shape, jnp.float32)
    total, ours = lax.fori_loop(0, everyone, gather, (zero, zero))
    cells = rows * slabs * width
    reflected_ref[...] = ours / cells
    mean_ref[...] = total / cells / groups


def one_point(bloch, material, permittivity, peak, sheet, waveform, electric, magnetic):
    rows, width, depth = material.shape
    snaps = waveform.shape[0] // INTERVAL
    everyone = lax.axis_size("ka") * lax.axis_size("sp")
    hbm = pl.BlockSpec(memory_space=pltpu.HBM)
    lines = -(-snaps // 8) * 8
    vmem = pl.BlockSpec(memory_space=pltpu.VMEM)
    plane = (2, 4, width, depth)
    f32 = jnp.float32
    return pl.pallas_call(
        kernel,
        out_shape=(
            jax.ShapeDtypeStruct(electric.shape, f32),
            jax.ShapeDtypeStruct(magnetic.shape, f32),
            jax.ShapeDtypeStruct((lines, depth), f32),
            jax.ShapeDtypeStruct((lines, depth), f32),
        ),
        in_specs=[hbm] * 8,
        out_specs=(vmem, vmem, vmem, vmem),
        scratch_shapes=[
            pltpu.SMEM(bloch.shape, jnp.int32),
            pltpu.SMEM(permittivity.shape, f32),
            pltpu.SMEM(peak.shape, f32),
            pltpu.SMEM(waveform.shape, f32),
            pltpu.VMEM(material.shape, jnp.int32),
            pltpu.VMEM(sheet.shape, f32),
            pltpu.VMEM(electric.shape, electric.dtype),
            pltpu.VMEM(magnetic.shape, magnetic.dtype),
            pltpu.VMEM((lines, depth), f32),
            pltpu.VMEM((everyone, lines, depth), f32),
            pltpu.VMEM((rows, width, depth), f32),
            pltpu.VMEM((rows, width, depth), f32),
            pltpu.VMEM((2, rows, width, depth), f32),
            pltpu.VMEM(plane, f32),
            pltpu.VMEM(plane, f32),
            pltpu.VMEM(plane, f32),
            pltpu.VMEM(plane, f32),
            pltpu.SemaphoreType.DMA((2,)),
            pltpu.SemaphoreType.DMA((2,)),
            pltpu.SemaphoreType.DMA((2,)),
            pltpu.SemaphoreType.DMA((2,)),
            pltpu.SemaphoreType.DMA((12,)),
            pltpu.SemaphoreType.DMA,
            pltpu.SemaphoreType.DMA,
        ],
        compiler_params=pltpu.CompilerParams(
            collective_id=0, has_side_effects=True, vmem_limit_bytes=40 * 1024 * 1024
        ),
    )(bloch, permittivity, peak, waveform, material, sheet, electric, magnetic)


def on_device(
    bloch_index,
    material,
    permittivity,
    absorption_peak,
    source_sheet,
    waveform,
    electric_in,
    magnetic_in,
):
    points = bloch_index.shape[0]
    results = [
        one_point(
            bloch_index[p : p + 1],
            material,
            permittivity,
            absorption_peak,
            source_sheet[p : p + 1],
            waveform,
            electric_in[p : p + 1],
            magnetic_in[p : p + 1],
        )
        for p in range(points)
    ]
    electric_out = jnp.concatenate([r[0] for r in results], 0)
    magnetic_out = jnp.concatenate([r[1] for r in results], 0)
    snaps = waveform.shape[0] // INTERVAL
    reflected = jnp.stack([r[2][:snaps, PML + 6] for r in results], 0)
    reflected_mean = sum(r[3][:snaps, PML + 6] for r in results) / points
    return (electric_out, magnetic_out, reflected, reflected_mean)


def solution(mesh):
    in_specs = (
        P("ka", None),
        P("sp", None, None),
        P(),
        P(),
        P("ka", None, "sp", None),
        P(),
        P("ka", None, "sp", None, None),
        P("ka", None, "sp", None, None),
    )
    out_specs = (
        P("ka", None, "sp", None, None),
        P("ka", None, "sp", None, None),
        P("ka", None),
        P(),
    )
    return jax.shard_map(
        on_device, mesh=mesh, in_specs=in_specs, out_specs=out_specs, check_vma=False
    )
```

```python
import jax
import jax.numpy as jnp
from jax import lax
from jax.experimental import pallas as pl
from jax.experimental.pallas import tpu as pltpu
from jax.sharding import PartitionSpec as P

PML = 16
INTERVAL = 5
MPHASE = 64
NMAT = 3
TIME_STEP = 0.5
MESH = pl.DeviceIdType.MESH


def rotate(couple, cosine, sine):
    return (couple[0] * cosine - couple[1] * sine, couple[0] * sine + couple[1] * cosine)


def minus(left, right):
    return (left[0] - right[0], left[1] - right[1])


def plus(left, right):
    return (left[0] + right[0], left[1] + right[1])


def relax(couple, change, keep, gain):
    return tuple(keep * c + gain * d for c, d in zip(couple, change))


def kernel(
    bloch_in,
    perm_in,
    peak_in,
    wave_in,
    material_in,
    sheet_in,
    e_hbm,
    h_hbm,
    e_ref,
    h_ref,
    reflected_ref,
    mean_ref,
    bloch_ref,
    perm_ref,
    peak_ref,
    wave_ref,
    material_ref,
    sheet_ref,
    e_in,
    h_in,
    report_ref,
    got_report,
    keep_ref,
    gain_ref,
    drive_ref,
    out_e,
    out_w,
    got_e,
    got_w,
    send_e,
    send_w,
    recv_e,
    recv_w,
    load_sem,
    send_report,
    recv_report,
):
    rows, width, depth = material_ref.shape
    steps = wave_ref.shape[0]
    slabs = lax.axis_size("sp")
    slab = lax.axis_index("sp")
    upper = lax.rem(slab + 1, slabs)
    lower = lax.rem(slab + slabs - 1, slabs)

    groups = lax.axis_size("ka")
    group = lax.axis_index("ka")
    everyone = groups * slabs
    me = group * slabs + slab

    def place(at):
        return {"ka": lax.div(at, slabs), "sp": lax.rem(at, slabs)}

    last_row = rows - 1
    loads = [
        pltpu.make_async_copy(src, dst, load_sem.at[at])
        for at, (src, dst) in enumerate(
            (
                (e_hbm.at[0, :, last_row], e_in.at[0, :, last_row]),
                (h_hbm.at[0, :, last_row], h_in.at[0, :, last_row]),
                (e_hbm.at[0, :, 0], e_in.at[0, :, 0]),
                (h_hbm.at[0, :, 0], h_in.at[0, :, 0]),
                (bloch_in, bloch_ref),
                (perm_in, perm_ref),
                (peak_in, peak_ref),
                (wave_in, wave_ref),
                (e_hbm.at[0, :, 1:last_row], e_in.at[0, :, 1:last_row]),
                (h_hbm.at[0, :, 1:last_row], h_in.at[0, :, 1:last_row]),
                (material_in, material_ref),
                (sheet_in, sheet_ref),
            )
        )
    ]
    for load in loads:
        load.start()

    barrier = pltpu.get_barrier_semaphore()

    def greet(offset, carry):
        other = lax.rem(me + offset, everyone)
        pl.semaphore_signal(barrier, inc=1, device_id=place(other), device_id_type=MESH)
        return carry

    lax.fori_loop(1, everyone, greet, 0)
    for load in loads[4:8]:
        load.wait()

    height = lax.broadcasted_iota(jnp.int32, (8, depth), 1).astype(jnp.float32)
    low_depth = jnp.maximum(PML - height, 0.0) / PML
    high_depth = jnp.maximum(height - (depth - 1 - PML), 0.0) / PML
    conduct = peak_ref[0] * (
        low_depth * low_depth * low_depth + high_depth * high_depth * high_depth
    )
    half_mag = conduct * (0.5 * TIME_STEP)
    h_keep = ((1.0 - half_mag) / (1.0 + half_mag))[0:1]
    h_gain = (-TIME_STEP / (1.0 + half_mag))[0:1]
    tables = []
    for level in range(NMAT):
        relative = jnp.full((8, depth), perm_ref[level], jnp.float32)
        half_ele = conduct * (0.5 * TIME_STEP) / relative
        tables.append(
            (
                ((1.0 - half_ele) / (1.0 + half_ele))[0:1],
                (TIME_STEP / relative / (1.0 + half_ele))[0:1],
            )
        )

    def trig(member):
        angle = jnp.full((8, depth), bloch_ref[0, member], jnp.int32).astype(jnp.float32)
        angle = 2.0 * jnp.pi * angle / MPHASE
        return jnp.cos(angle)[0:1], jnp.sin(angle)[0:1]

    cos_x, sin_x = trig(0)
    cos_y, sin_y = trig(1)
    at_end = (slab == slabs - 1).astype(jnp.float32)
    at_start = (slab == 0).astype(jnp.float32)
    end_cos = at_end * cos_x + (1.0 - at_end)
    end_sin = at_end * sin_x
    start_cos = at_start * cos_x + (1.0 - at_start)
    start_sin = -at_start * sin_x

    lane = lax.broadcasted_iota(jnp.int32, (width, depth), 1)
    last_lane = lane == depth - 1
    first_lane = lane == 0
    sub = lax.broadcasted_iota(jnp.int32, (8, depth), 0)

    def above_z(couple):
        return tuple(jnp.where(last_lane, 0.0, pltpu.roll(v, depth - 1, 1)) for v in couple)

    def below_z(couple):
        return tuple(jnp.where(first_lane, 0.0, pltpu.roll(v, 1, 1)) for v in couple)

    def above_y(couple):
        moved = tuple(pltpu.roll(v, width - 1, 0) for v in couple)
        tail = tuple(v[width - 8 :] for v in moved)
        turned = rotate(tail, cos_y, sin_y)
        return tuple(
            jnp.concatenate([v[: width - 8], jnp.where(sub == 7, r, w)], axis=0)
            for v, r, w in zip(moved, turned, tail)
        )

    def below_y(couple):
        moved = tuple(pltpu.roll(v, 1, 0) for v in couple)
        head = tuple(v[:8] for v in moved)
        turned = rotate(head, cos_y, -sin_y)
        return tuple(
            jnp.concatenate([jnp.where(sub == 0, r, w), v[8:]], axis=0)
            for v, r, w in zip(moved, turned, head)
        )

    def get(ref, member, x):
        return (ref[0, 2 * member, x], ref[0, 2 * member + 1, x])

    def put(ref, member, x, couple):
        ref[0, 2 * member, x] = couple[0]
        ref[0, 2 * member + 1, x] = couple[1]

    def get_plane(ref, slot, member):
        return (ref[slot, 2 * member], ref[slot, 2 * member + 1])

    def put_plane(ref, slot, member, couple):
        ref[slot, 2 * member] = couple[0]
        ref[slot, 2 * member + 1] = couple[1]

    def hx_plane(x):
        ey, ez = get(e_ref, 1, x), get(e_ref, 2, x)
        change = minus(minus(above_y(ez), ez), minus(above_z(ey), ey))
        put(h_ref, 0, x, relax(get(h_ref, 0, x), change, h_keep, h_gain))

    def h_plane(x, carry):
        hx_plane(x)
        ex, ey, ez = get(e_ref, 0, x), get(e_ref, 1, x), get(e_ref, 2, x)
        dx_ez = minus(get(e_ref, 2, x + 1), ez)
        dx_ey = minus(get(e_ref, 1, x + 1), ey)
        change = minus(minus(above_z(ex), ex), dx_ez)
        put(h_ref, 1, x, relax(get(h_ref, 1, x), change, h_keep, h_gain))
        change = minus(dx_ey, minus(above_y(ex), ex))
        put(h_ref, 2, x, relax(get(h_ref, 2, x), change, h_keep, h_gain))
        return carry

    def partial_h(slot):
        x = rows - 1
        ex, ey, ez = get(e_ref, 0, x), get(e_ref, 1, x), get(e_ref, 2, x)
        change = plus(minus(above_z(ex), ex), ez)
        put_plane(out_w, slot, 0, relax(get(h_ref, 1, x), change, h_keep, h_gain))
        change = minus(minus(ex, above_y(ex)), ey)
        put_plane(out_w, slot, 1, relax(get(h_ref, 2, x), change, h_keep, h_gain))

    def complete_h(slot):
        x = rows - 1
        beyond_y = rotate(get_plane(got_e, slot, 0), end_cos, end_sin)
        beyond_z = rotate(get_plane(got_e, slot, 1), end_cos, end_sin)
        w_y, w_z = get_plane(out_w, slot, 0), get_plane(out_w, slot, 1)
        put(h_ref, 1, x, tuple(w - h_gain * b for w, b in zip(w_y, beyond_z)))
        put(h_ref, 2, x, tuple(w + h_gain * b for w, b in zip(w_z, beyond_y)))

    def e_update(x, drive, hy_prev, hz_prev):
        hx, hy, hz = get(h_ref, 0, x), get(h_ref, 1, x), get(h_ref, 2, x)
        keep, gain = keep_ref[x], gain_ref[x]
        change = minus(minus(hz, below_y(hz)), minus(hy, below_z(hy)))
        change = (change[0] - drive * drive_ref[0, x], change[1] - drive * drive_ref[1, x])
        put(e_ref, 0, x, relax(get(e_ref, 0, x), change, keep, gain))
        change = minus(minus(hx, below_z(hx)), minus(hz, hz_prev))
        ey = relax(get(e_ref, 1, x), change, keep, gain)
        put(e_ref, 1, x, ey)
        change = minus(minus(hy, hy_prev), minus(hx, below_y(hx)))
        ez = relax(get(e_ref, 2, x), change, keep, gain)
        put(e_ref, 2, x, ez)
        return ey, ez

    def e_first(slot, drive):
        ey, ez = get(e_ref, 1, 0), get(e_ref, 2, 0)
        turned_y = rotate(get_plane(got_w, slot, 0), start_cos, start_sin)
        turned_z = rotate(get_plane(got_w, slot, 1), start_cos, start_sin)
        hy_prev = tuple(w - h_gain * e for w, e in zip(turned_y, ez))
        hz_prev = tuple(w + h_gain * e for w, e in zip(turned_z, ey))
        return e_update(0, drive, hy_prev, hz_prev)

    def copy_e(slot):
        return pltpu.make_async_remote_copy(
            src_ref=out_e.at[slot],
            dst_ref=got_e.at[slot],
            send_sem=send_e.at[slot],
            recv_sem=recv_e.at[slot],
            device_id={"sp": lower},
            device_id_type=MESH,
        )

    def copy_w(slot):
        return pltpu.make_async_remote_copy(
            src_ref=out_w.at[slot],
            dst_ref=got_w.at[slot],
            send_sem=send_w.at[slot],
            recv_sem=recv_w.at[slot],
            device_id={"sp": upper},
            device_id_type=MESH,
        )

    def widen(x, carry):
        for member in range(6):
            e_ref[0, member, x] = e_in[0, member, x].astype(jnp.float32)
            h_ref[0, member, x] = h_in[0, member, x].astype(jnp.float32)
        return carry

    for load in loads[0:4]:
        load.wait()
    widen(rows - 1, 0)
    partial_h(0)
    widen(0, 0)
    for member in range(2):
        put_plane(out_e, 0, member, get(e_ref, 1 + member, 0))
    pl.semaphore_wait(barrier, everyone - 1)
    copy_w(0).start()
    copy_e(0).start()
    for load in loads[8:]:
        load.wait()
    lax.fori_loop(1, rows - 1, widen, 0)

    report_ref[...] = jnp.zeros_like(report_ref)
    square = lax.broadcasted_iota(jnp.int32, (width, width), 0) == lax.broadcasted_iota(
        jnp.int32, (width, width), 1
    )

    def prepare(x, carry):
        kind = material_ref[x]
        keep, gain = tables[0]
        for level in range(1, NMAT):
            keep = jnp.where(kind == level, tables[level][0], keep)
            gain = jnp.where(kind == level, tables[level][1], gain)
        keep_ref[x] = keep
        gain_ref[x] = gain
        for part in range(2):
            row = sheet_ref[0, part, pl.ds(x, 1), :]
            column = jnp.sum(jnp.where(square, row, 0.0), axis=1, keepdims=True)
            drive_ref[part, x] = jnp.where(lane == PML + 2, column, 0.0)
        return carry

    lax.fori_loop(0, rows, prepare, 0)

    def power(x, total):
        for member in range(4):
            value = e_ref[0, member, x]
            total = total + value * value
        return total

    def step(t, carry):
        slot = lax.rem(t, 2)
        later = lax.rem(t + 1, 2)
        drive = wave_ref[t]
        even = slot == 0
        ready = jnp.logical_and(t >= 1, t < steps - 1)
        snapshot = lax.rem(t + 1, INTERVAL) == 0
        empty = jnp.zeros((width, depth), jnp.float32)

        def left():
            copy_w(slot).wait_recv()
            ey, ez = e_first(slot, drive)

            @pl.when(ready)
            def _():
                copy_e(later).wait_send()

            @pl.when(t < steps - 1)
            def _():
                put_plane(out_e, later, 0, ey)
                put_plane(out_e, later, 1, ez)
                copy_e(later).start()

        def right():
            copy_e(slot).wait_recv()
            complete_h(slot)
            e_update(rows - 1, drive, get(h_ref, 1, rows - 2), get(h_ref, 2, rows - 2))

            @pl.when(ready)
            def _():
                copy_w(later).wait_send()

            @pl.when(t < steps - 1)
            def _():
                partial_h(later)
                copy_w(later).start()

        def inner(x, held):
            e_update(x, drive, get(h_ref, 1, x - 1), get(h_ref, 2, x - 1))
            return held

        lax.fori_loop(0, rows - 1, h_plane, 0)
        hx_plane(rows - 1)
        pl.when(even)(left)
        pl.when(jnp.logical_not(even))(right)
        lax.fori_loop(1, rows - 1, inner, 0)

        @pl.when(snapshot)
        def _():
            total = lax.fori_loop(1, rows - 1, power, empty)
            report_ref[pl.ds(lax.div(t, INTERVAL), 1)] = jnp.sum(total, axis=0, keepdims=True)

        pl.when(even)(right)
        pl.when(jnp.logical_not(even))(left)

        @pl.when(snapshot)
        def _():
            total = power(0, power(rows - 1, empty))
            at = lax.div(t, INTERVAL)
            report_ref[pl.ds(at, 1)] += jnp.sum(total, axis=0, keepdims=True)

        return carry

    lax.fori_loop(0, steps, step, 0)

    def tell(offset):
        return pltpu.make_async_remote_copy(
            src_ref=report_ref,
            dst_ref=got_report.at[me],
            send_sem=send_report,
            recv_sem=recv_report,
            device_id=place(lax.rem(me + offset, everyone)),
            device_id_type=MESH,
        )

    def tell_start(offset, carry):
        tell(offset).start()
        return carry

    lax.fori_loop(1, everyone, tell_start, 0)
    got_report[me] = report_ref[...]
    for t in (steps - 2, steps - 1):
        copy_e(t % 2).wait_send()
        copy_w(t % 2).wait_send()
    everything = got_report.at[pl.ds(0, everyone - 1)]
    pltpu.make_async_copy(everything, everything, recv_report).wait()
    pltpu.make_async_copy(everything, everything, send_report).wait()

    def gather(at, held):
        value = got_report[at]
        ours = (lax.div(at, slabs) == group).astype(jnp.float32)
        return held[0] + value, held[1] + ours * value

    zero = jnp.zeros(report_ref.shape, jnp.float32)
    total, ours = lax.fori_loop(0, everyone, gather, (zero, zero))
    cells = rows * slabs * width
    reflected_ref[...] = ours / cells
    mean_ref[...] = total / cells / groups


def one_point(bloch, material, permittivity, peak, sheet, waveform, electric, magnetic):
    rows, width, depth = material.shape
    snaps = waveform.shape[0] // INTERVAL
    everyone = lax.axis_size("ka") * lax.axis_size("sp")
    hbm = pl.BlockSpec(memory_space=pltpu.HBM)
    lines = -(-snaps // 8) * 8
    vmem = pl.BlockSpec(memory_space=pltpu.VMEM)
    plane = (2, 4, width, depth)
    f32 = jnp.float32
    return pl.pallas_call(
        kernel,
        out_shape=(
            jax.ShapeDtypeStruct(electric.shape, f32),
            jax.ShapeDtypeStruct(magnetic.shape, f32),
            jax.ShapeDtypeStruct((lines, depth), f32),
            jax.ShapeDtypeStruct((lines, depth), f32),
        ),
        in_specs=[hbm] * 8,
        out_specs=(vmem, vmem, vmem, vmem),
        scratch_shapes=[
            pltpu.SMEM(bloch.shape, jnp.int32),
            pltpu.SMEM(permittivity.shape, f32),
            pltpu.SMEM(peak.shape, f32),
            pltpu.SMEM(waveform.shape, f32),
            pltpu.VMEM(material.shape, jnp.int32),
            pltpu.VMEM(sheet.shape, f32),
            pltpu.VMEM(electric.shape, electric.dtype),
            pltpu.VMEM(magnetic.shape, magnetic.dtype),
            pltpu.VMEM((lines, depth), f32),
            pltpu.VMEM((everyone, lines, depth), f32),
            pltpu.VMEM((rows, width, depth), f32),
            pltpu.VMEM((rows, width, depth), f32),
            pltpu.VMEM((2, rows, width, depth), f32),
            pltpu.VMEM(plane, f32),
            pltpu.VMEM(plane, f32),
            pltpu.VMEM(plane, f32),
            pltpu.VMEM(plane, f32),
            pltpu.SemaphoreType.DMA((2,)),
            pltpu.SemaphoreType.DMA((2,)),
            pltpu.SemaphoreType.DMA((2,)),
            pltpu.SemaphoreType.DMA((2,)),
            pltpu.SemaphoreType.DMA((12,)),
            pltpu.SemaphoreType.DMA,
            pltpu.SemaphoreType.DMA,
        ],
        compiler_params=pltpu.CompilerParams(
            collective_id=0, has_side_effects=True, vmem_limit_bytes=40 * 1024 * 1024
        ),
    )(*((v if v.shape == (1,) else pltpu.with_memory_space_constraint(v, pltpu.HBM)) for v in (bloch, permittivity, peak, waveform, material, sheet, electric, magnetic)))


def on_device(
    bloch_index,
    material,
    permittivity,
    absorption_peak,
    source_sheet,
    waveform,
    electric_in,
    magnetic_in,
):
    points = bloch_index.shape[0]
    results = [
        one_point(
            bloch_index[p : p + 1],
            material,
            permittivity,
            absorption_peak,
            source_sheet[p : p + 1],
            waveform,
            electric_in[p : p + 1],
            magnetic_in[p : p + 1],
        )
        for p in range(points)
    ]
    electric_out = jnp.concatenate([r[0] for r in results], 0)
    magnetic_out = jnp.concatenate([r[1] for r in results], 0)
    snaps = waveform.shape[0] // INTERVAL
    reflected = jnp.stack([r[2][:snaps, PML + 6] for r in results], 0)
    reflected_mean = sum(r[3][:snaps, PML + 6] for r in results) / points
    return (electric_out, magnetic_out, reflected, reflected_mean)


def solution(mesh):
    in_specs = (
        P("ka", None),
        P("sp", None, None),
        P(),
        P(),
        P("ka", None, "sp", None),
        P(),
        P("ka", None, "sp", None, None),
        P("ka", None, "sp", None, None),
    )
    out_specs = (
        P("ka", None, "sp", None, None),
        P("ka", None, "sp", None, None),
        P("ka", None),
        P(),
    )
    return jax.shard_map(
        on_device, mesh=mesh, in_specs=in_specs, out_specs=out_specs, check_vma=False
    )
```
